16 devices in a mesh: ty: 4 (over z, y), tx: 4 (over x, core).
Axes of the slice: x: 2, y: 2, z: 2, core: 2. Of those that a mesh axis runs over, the one named last changes fastest.
Arguments:
- w_in: float32 [4, 4, 4, 384, 1536], P('tx', 'ty')
- w_out: float32 [4, 4, 4, 1536, 384], P('tx', 'ty')
- inputs: bfloat16 [4, 4, 4, 4096, 384], P('tx', 'ty')
- targets: bfloat16 [4, 4, 4, 4096, 384], P('tx', 'ty')
Outputs:
- output 1: float32 [4, 4, 4, 384, 1536], P('tx', 'ty')
- output 2: float32 [4, 4, 4, 1536, 384], P('tx', 'ty')
- output 3: float32 [4, 4, 4, 384, 1536], P('tx', 'ty')
- output 4: float32 [4, 4, 4, 1536, 384], P('tx', 'ty')
All inputs are finite; a program needn't handle non-finite values.
Results may differ from the reference program's by a relative error of at most 0.00533436.
Values are sent between devices in bfloat16 or wider.
A program may use at most 1 GiB of HBM per device.

```python
import jax
import jax.numpy as jnp
from jax import lax

TX = 4
TY = 4
LAYERS = 4
D = 384
FF = 1536
ROWS = 4096
STEPS = 3
EPS = 1e-6
LEARN_RATE = 0.125


def setup_inputs(seed: int = 0) -> dict:
    root_key = jax.random.key(seed)
    key_list = jax.random.split(root_key, 6)
    base_in = jax.random.normal(key_list[0], (LAYERS, D, FF), jnp.float32)
    own_in = jax.random.normal(key_list[1], (TX, TY, LAYERS, D, FF), jnp.float32)
    w_in = (base_in[None, None] + 0.5 * own_in) * (D ** -0.5)
    base_out = jax.random.normal(key_list[2], (LAYERS, FF, D), jnp.float32)
    own_out = jax.random.normal(key_list[3], (TX, TY, LAYERS, FF, D), jnp.float32)
    w_out = (base_out[None, None] + 0.5 * own_out) * (FF ** -0.5)
    inputs = jax.random.normal(key_list[4], (TX, TY, STEPS + 1, ROWS, D), jnp.float32).astype(jnp.bfloat16)
    targets = jax.random.normal(key_list[5], (TX, TY, STEPS + 1, ROWS, D), jnp.float32).astype(jnp.bfloat16)
    return {'w_in': w_in, 'w_out': w_out, 'inputs': inputs, 'targets': targets}


def layer_step(hidden, weights):
    mat_in, mat_out = weights
    hidden_f32 = hidden.astype(jnp.float32)
    inv_rms = lax.rsqrt(jnp.mean(hidden_f32 * hidden_f32, axis=-1, keepdims=True) + EPS)
    normed = (hidden_f32 * inv_rms).astype(jnp.bfloat16)
    pre_act = jnp.dot(normed, mat_in.astype(jnp.bfloat16), preferred_element_type=jnp.float32)
    gelu_out = jax.nn.gelu(pre_act).astype(jnp.bfloat16)
    mlp_out = jnp.dot(gelu_out, mat_out.astype(jnp.bfloat16), preferred_element_type=jnp.float32)
    return (hidden_f32 + mlp_out).astype(jnp.bfloat16), None


def local_loss(w_in, w_out, batch_in, batch_tgt):
    last_hidden, _ = lax.scan(layer_step, batch_in, (w_in, w_out))
    resid_err = last_hidden.astype(jnp.float32) - batch_tgt.astype(jnp.float32)
    return jnp.mean(resid_err * resid_err)


local_grads = jax.grad(local_loss, argnums=(0, 1))


def gossip_mix(values):
    sent_copy = values.astype(jnp.bfloat16).astype(jnp.float32)
    summed = values + jnp.roll(sent_copy, 1, axis=0)
    summed = summed + jnp.roll(sent_copy, -1, axis=0)
    summed = summed + jnp.roll(sent_copy, 1, axis=1)
    summed = summed + jnp.roll(sent_copy, -1, axis=1)
    return summed / 5.0


def reference(w_in, w_out, inputs, targets):
    cell_count = TX * TY
    step_size = LEARN_RATE

    def one_cell(operands):
        return local_grads(operands[0], operands[1], operands[2], operands[3])

    def all_grads(p_in, p_out, step_idx):
        batch_in = lax.dynamic_index_in_dim(inputs, step_idx, axis=2, keepdims=False).reshape((cell_count, ROWS, D))
        batch_tgt = lax.dynamic_index_in_dim(targets, step_idx, axis=2, keepdims=False).reshape((cell_count, ROWS, D))
        grad_in, grad_out = lax.map(one_cell, (p_in.reshape((cell_count, LAYERS, D, FF)), p_out.reshape((cell_count, LAYERS, FF, D)), batch_in, batch_tgt))
        return grad_in.reshape(p_in.shape), grad_out.reshape(p_out.shape)

    first_in, first_out = all_grads(w_in, w_out, 0)

    def step_body(carried, step_idx):
        p_in, p_out, y_in, y_out, old_in, old_out = carried
        p_in = gossip_mix(p_in) - step_size * y_in
        p_out = gossip_mix(p_out) - step_size * y_out
        new_gin, new_gout = all_grads(p_in, p_out, step_idx)
        y_in = gossip_mix(y_in) + new_gin - old_in
        y_out = gossip_mix(y_out) + new_gout - old_out
        return (p_in, p_out, y_in, y_out, new_gin, new_gout), None

    final_state, _ = lax.scan(step_body, (w_in, w_out, first_in, first_out, first_in, first_out), jnp.arange(1, STEPS + 1))
    return (final_state[0], final_state[1], final_state[2], final_state[3])
```

```python
import functools

import jax
import jax.numpy as jnp
import numpy as np
from jax import lax
from jax.experimental import pallas as pl
from jax.experimental.pallas import tpu as pltpu
from jax.sharding import PartitionSpec as P

bf16, f32 = jnp.bfloat16, jnp.float32
EPS = 1e-6
LEARN_RATE = 0.125
GELU_A = float(np.sqrt(2 / np.pi))
GELU_B = GELU_A * 0.044715
TILE = 512
COLS = 768
SUB = 96
CORE, XDIR, YDIR, ZDIR = range(4)


def dot_nt(a, b):
    return lax.dot_general(a, b, (((1,), (1,)), ((), ())), preferred_element_type=f32)


def dot_nn(a, b):
    return jnp.dot(a, b, preferred_element_type=f32)


def step_kernel(step, last, names, *refs):
    r = dict(zip(names, refs))
    first = step == 0
    x_ref, t_ref, nb, w, dw = r['x'], r['t'], r['nb'], r['w'], r['dw']
    mats, d, ff = w.shape
    rows = x_ref.shape[1]
    tiles = rows // TILE
    subs = d // SUB
    chunks = mats * subs
    send_sem, recv_sem = r['send_sem'], r['recv_sem']
    sets = nb.shape[0]
    p_set = None if last else sets - 1
    y_set = None if first else 0

    tx, ty = lax.axis_index('tx'), lax.axis_index('ty')
    peers = (
        {'tx': tx + 1 - 2 * lax.rem(tx, 2)},
        {'tx': 3 - tx},
        {'ty': ty + 1 - 2 * lax.rem(ty, 2)},
        {'ty': lax.rem(ty + 2, 4)},
    )
    xpar, ypar = lax.rem(tx, 2), lax.rem(ty, 2)
    order = (1 - xpar, xpar, 3 - ypar, 2 + ypar)

    def remote(src, group, direction, mat):
        slot = group * mats + mat
        return pltpu.make_async_remote_copy(
            src_ref=src, dst_ref=nb.at[group, direction, mat],
            send_sem=send_sem.at[direction, slot], recv_sem=recv_sem.at[direction, slot],
            device_id=peers[direction], device_id_type=pl.DeviceIdType.MESH)

    def send(src, group, mat):
        for direction in (YDIR, XDIR, CORE):
            remote(src.at[mat], group, direction, mat).start()

    def arrived(group, direction, mat):
        remote(nb.at[group, direction, mat], group, direction, mat).wait_recv()

    def forward(slot):
        group, mat = lax.div(slot, mats), lax.rem(slot, mats)
        arrived(group, YDIR, mat)
        remote(nb.at[group, YDIR, mat], group, ZDIR, mat).start()

    def where(q):
        return lax.div(q, subs), pl.ds(pl.multiple_of(lax.rem(q, subs) * SUB, SUB), SUB)

    def stream(ins, outs, body, before=None):
        def get(q, slot):
            mat, rng = where(q)
            return [pltpu.make_async_copy(src(mat, rng), buf.at[slot], r['in_sem'].at[k, slot])
                    for k, (src, buf) in enumerate(ins)]

        def put(q, slot):
            mat, rng = where(q)
            return [pltpu.make_async_copy(buf.at[slot], dst(mat, rng), r['out_sem'].at[k, slot])
                    for k, (buf, dst) in enumerate(outs)]

        if before is not None:
            before(0)
        for c in get(0, 0):
            c.start()

        def one(q, carry):
            slot = lax.rem(q, 2)

            @pl.when(q + 1 < chunks)
            def _():
                if before is not None:
                    @pl.when(lax.rem(q + 1, subs) == 0)
                    def _():
                        before(lax.div(q + 1, subs))
                for c in get(q + 1, 1 - slot):
                    c.start()
            for c in get(q, slot):
                c.wait()

            @pl.when(q >= 2)
            def _():
                for c in put(q - 2, slot):
                    c.wait()
            body(q, slot)
            for c in put(q, slot):
                c.start()
            return carry

        lax.fori_loop(0, chunks, one, 0)
        for q in (chunks - 2, chunks - 1):
            for c in put(q, q % 2):
                c.wait()

    def mix(v, bn, slot):
        for k in range(4):
            v = v + bn[k, slot].astype(f32)
        return v / 5.0

    def neighbour(source, group, k):
        return lambda mat, rng: source.at[group, order[k], mat, rng]

    if not first:
        def send_y(mat, carry):
            send(r['y_send'], y_set, mat)
            return carry
        lax.fori_loop(0, mats, send_y, 0)

    def late_send(q):
        if p_set is not None:
            @pl.when(jnp.logical_and(lax.rem(q, subs) == 0, q > 0))
            def _():
                send(w, p_set, lax.div(q, subs) - 1)

    if first:
        def load_weights(bp):
            def body(q, slot):
                mat, rng = where(q)
                w[mat, rng, :] = bp[slot].astype(bf16)
                late_send(q)
            stream([(lambda mat, rng: r['p'].at[mat, rng], bp)], [], body)
        pl.run_scoped(load_weights, pltpu.VMEM((2, SUB, ff), f32))
    else:
        def new_weights(bp, bn, by, bo):
            def body(q, slot):
                mat, rng = where(q)
                pn = mix(bp[slot], bn, slot) - LEARN_RATE * by[slot].astype(f32)
                bo[slot] = pn
                w[mat, rng, :] = pn.astype(bf16)
                late_send(q)
            pnb = r['p_nb']
            ins = [(lambda mat, rng: r['p'].at[mat, rng], bp)]
            ins += [(neighbour(pnb, pnb.shape[0] - 1, k), bn.at[k]) for k in range(4)]
            ins += [(lambda mat, rng: r['y'].at[mat, rng], by)]
            stream(ins, [(bo, lambda mat, rng: r['p_out'].at[mat, rng])], body)
        pl.run_scoped(new_weights, pltpu.VMEM((2, SUB, ff), f32), pltpu.VMEM((4, 2, SUB, ff), bf16),
                      pltpu.VMEM((2, SUB, ff), r['y'].dtype), pltpu.VMEM((2, SUB, ff), f32))

    def zero(k, carry):
        dw[lax.div(k, subs), where(k)[1], :] = jnp.zeros((SUB, ff), f32)
        return carry
    lax.fori_loop(0, chunks, zero, 0)
    if p_set is not None:
        send(w, p_set, mats - 1)

    layers = mats // 2
    inv_count = 1.0 / (rows * d)

    def gradient(xb, tb, h_s, a_s, gp_s, dh_s):
        def fetch(i, slot):
            rng = pl.ds(pl.multiple_of(i * TILE, TILE), TILE)
            return (pltpu.make_async_copy(x_ref.at[step, rng], xb.at[slot], r['tile_sem'].at[0, slot]),
                    pltpu.make_async_copy(t_ref.at[step, rng], tb.at[slot], r['tile_sem'].at[1, slot]))
        for c in fetch(0, 0):
            c.start()

        def tile(i, carry):
            slot = lax.rem(i, 2)
            if first:
                @pl.when(i > 0)
                def _():
                    forward(i - 1)
            else:
                forward(i)
            for c in fetch(i, slot):
                c.wait()

            @pl.when(i + 1 < tiles)
            def _():
                for c in fetch(i + 1, 1 - slot):
                    c.start()
            h_s[0] = xb[slot]

            def fwd(l, carry):
                h = h_s[l].astype(f32)
                inv = lax.rsqrt(jnp.mean(h * h, axis=-1, keepdims=True) + EPS)
                u = (h * inv).astype(bf16)
                acc = jnp.zeros((TILE, d), f32)
                for c in range(0, ff, COLS):
                    cs = slice(c, c + COLS)
                    z = dot_nn(u, w[2 * l, :, cs])
                    z2 = z * z
                    th = jnp.tanh(z * (GELU_A + GELU_B * z2))
                    s = 0.5 + 0.5 * th
                    a = (z * s).astype(bf16)
                    a_s[l, :, cs] = a
                    gp_s[l, :, cs] = s + (z * (0.5 * GELU_A + 1.5 * GELU_B * z2)) * (1.0 - th * th)
                    acc = acc + dot_nt(a, w[2 * l + 1, :, cs])
                h_s[l + 1] = (h + acc).astype(bf16)
                return carry
            lax.fori_loop(0, layers, fwd, 0)

            err = h_s[layers].astype(f32) - tb[slot].astype(f32)
            dh_s[...] = ((err * inv_count) * 2.0).astype(bf16)

            def bwd(l, bottom):
                g = dh_s[...]
                g_t = g.T
                h = h_s[l].astype(f32)
                inv = lax.rsqrt(jnp.mean(h * h, axis=-1, keepdims=True) + EPS)
                u_t = (h * inv).astype(bf16).T
                du = jnp.zeros((TILE, d), f32)
                for c in range(0, ff, COLS):
                    cs = slice(c, c + COLS)
                    da = dot_nn(g, w[2 * l + 1, :, cs]).astype(bf16).astype(f32)
                    dz = (da * gp_s[l, :, cs]).astype(bf16)
                    dw[2 * l, :, cs] += dot_nn(u_t, dz)
                    dw[2 * l + 1, :, cs] += dot_nn(g_t, a_s[l, :, cs])
                    if not bottom:
                        du = du + dot_nt(dz, w[2 * l, :, cs])
                if not bottom:
                    du = du.astype(bf16).astype(f32)
                    dinv = jnp.sum(du * h, axis=-1, keepdims=True)
                    k = dinv * (inv * inv * inv) * (-1.0 / d)
                    dh_s[...] = (g.astype(f32) + du * inv + h * k).astype(bf16)

            def bwd_down(q, carry):
                bwd(layers - 1 - q, False)
                return carry
            lax.fori_loop(0, layers - 1, bwd_down, 0)
            bwd(0, True)
            return carry

        lax.fori_loop(0, tiles, tile, 0)

    pl.run_scoped(gradient, pltpu.VMEM((2, TILE, d), bf16), pltpu.VMEM((2, TILE, d), bf16),
                  pltpu.VMEM((layers + 1, TILE, d), bf16), pltpu.VMEM((layers, TILE, ff), bf16),
                  pltpu.VMEM((layers, TILE, ff), f32), pltpu.VMEM((TILE, d), bf16))

    sent = tiles - 1 if first else tiles
    slots = sets * mats
    if first:
        forward(sent)

        def new_tracker(og):
            def body(q, slot):
                mat, rng = where(q)
                og[slot] = dw[mat, rng, :].astype(bf16)
            stream([], [(og, lambda mat, rng: r['g_out'].at[mat, rng])], body)
        pl.run_scoped(new_tracker, pltpu.VMEM((2, SUB, ff), bf16))
    else:
        if not last:
            forward(sent)
            sent += 1
        same = 'g' not in r

        def new_tracker(bn, by, bg, bo, ob, og):
            def before(mat):
                for direction in (CORE, XDIR, ZDIR):
                    arrived(y_set, direction, mat)
                if not last:
                    @pl.when(mat == mats // 2)
                    def _():
                        forward(tiles + 1)

            def body(q, slot):
                mat, rng = where(q)
                g = dw[mat, rng, :].astype(bf16)
                old = (by if same else bg)[slot].astype(f32)
                y = (mix(by[slot].astype(f32), bn, slot) + g.astype(f32)) - old
                bo[slot] = y
                if not last:
                    ob[slot] = y.astype(bf16)
                    og[slot] = g
            ins = [(lambda mat, rng: r['y'].at[mat, rng], by)]
            ins += [(neighbour(nb, y_set, k), bn.at[k]) for k in range(4)]
            if not same:
                ins += [(lambda mat, rng: r['g'].at[mat, rng], bg)]
            outs = [(bo, lambda mat, rng: r['y_out'].at[mat, rng])]
            if not last:
                outs += [(ob, lambda mat, rng: r['yb_out'].at[mat, rng]),
                         (og, lambda mat, rng: r['g_out'].at[mat, rng])]
            stream(ins, outs, body, before)
        block = (2, SUB, ff)
        pl.run_scoped(new_tracker, pltpu.VMEM((4,) + block, bf16), pltpu.VMEM(block, r['y'].dtype), pltpu.VMEM(block, bf16),
                      pltpu.VMEM(block, f32), pltpu.VMEM(block, bf16), pltpu.VMEM(block, bf16))
        if not last:
            sent += 1

    if first:
        sent += 1

    def rest(slot, carry):
        forward(slot)
        return carry
    lax.fori_loop(sent, slots, rest, 0)

    def drain(slot, carry):
        group, mat = lax.div(slot, mats), lax.rem(slot, mats)
        for direction in range(4):
            remote(nb.at[group, direction, mat], group, direction, mat).wait_send()
        return carry
    lax.fori_loop(0, slots, drain, 0)
    if p_set is not None:
        def settle(mat, carry):
            for direction in (CORE, XDIR, ZDIR):
                arrived(p_set, direction, mat)
            return carry
        lax.fori_loop(0, mats, settle, 0)


def run_step(step, last, ins):
    mats, d, ff = ins['p'].shape
    first = step == 0
    sets = 1 if first or last else 2
    big = lambda dtype: jax.ShapeDtypeStruct((mats, d, ff), dtype)
    outs = {'nb': jax.ShapeDtypeStruct((sets, 4, mats, d, ff), bf16)}
    if first:
        outs['g_out'] = big(bf16)
    else:
        outs['p_out'] = big(f32)
        outs['y_out'] = big(f32)
        if not last:
            outs['yb_out'] = big(bf16)
            outs['g_out'] = big(bf16)
    scratch = {
        'w': pltpu.VMEM((mats, d, ff), bf16),
        'dw': pltpu.VMEM((mats, d, ff), f32),
        'send_sem': pltpu.SemaphoreType.DMA((4, sets * mats)),
        'recv_sem': pltpu.SemaphoreType.DMA((4, sets * mats)),
        'in_sem': pltpu.SemaphoreType.DMA((6, 2)),
        'out_sem': pltpu.SemaphoreType.DMA((3, 2)),
        'tile_sem': pltpu.SemaphoreType.DMA((2, 2)),
    }
    names = tuple(ins) + tuple(outs) + tuple(scratch)
    anywhere = pl.BlockSpec(memory_space=pl.ANY)
    res = pl.pallas_call(
        functools.partial(step_kernel, step, last, names),
        out_shape=tuple(outs.values()),
        in_specs=[anywhere] * len(ins),
        out_specs=tuple(anywhere for _ in outs),
        scratch_shapes=list(scratch.values()),
        compiler_params=pltpu.CompilerParams(vmem_limit_bytes=67043328, has_side_effects=True),
        name='step%d' % step,
    )(*ins.values())
    return dict(zip(outs, res))


def solution(mesh):
    def device_fn(w_in, w_out, inputs, targets):
        layers, d, ff = w_in.shape[2:]
        x, t = inputs[0, 0], targets[0, 0]
        steps = x.shape[0] - 1
        p = jnp.stack([w_in[0, 0], jnp.swapaxes(w_out[0, 0], 1, 2)], axis=1).reshape(2 * layers, d, ff)
        out = run_step(0, False, {'x': x, 't': t, 'p': p})
        y, y_send, g, p_nb = out['g_out'], out['g_out'], None, out['nb']
        for step in range(1, steps + 1):
            ins = {'x': x, 't': t, 'p': p, 'p_nb': p_nb, 'y': y}
            if g is None:
                ins['y_send'] = y_send
            else:
                ins['y_send'] = y_send
                ins['g'] = g
            out = run_step(step, step == steps, ins)
            p, y, p_nb = out['p_out'], out['y_out'], out['nb']
            if step < steps:
                y_send, g = out['yb_out'], out['g_out']

        def split(v):
            v = v.reshape(layers, 2, d, ff)
            return v[:, 0][None, None], jnp.swapaxes(v[:, 1], 1, 2)[None, None]
        return split(p) + split(y)

    spec = P('tx', 'ty')
    return jax.shard_map(device_fn, mesh=mesh, in_specs=(spec,) * 4, out_specs=(spec,) * 4, check_vma=False)
```

```python
import functools

import jax
import jax.numpy as jnp
import numpy as np
from jax import lax
from jax.experimental import pallas as pl
from jax.experimental.pallas import tpu as pltpu
from jax.sharding import PartitionSpec as P

bf16, f32 = jnp.bfloat16, jnp.float32
EPS = 1e-6
LEARN_RATE = 0.125
GELU_A = float(np.sqrt(2 / np.pi))
GELU_B = GELU_A * 0.044715
TILE = 512
COLS = 768
SUB = 128
DEPTH = 4
PARTS = 2
CORE, XDIR, YDIR, ZDIR = range(4)


def dot_nt(a, b):
    return lax.dot_general(a, b, (((1,), (1,)), ((), ())), preferred_element_type=f32)


def dot_nn(a, b):
    return jnp.dot(a, b, preferred_element_type=f32)


def where(q, subs):
    return lax.div(q, subs), pl.ds(pl.multiple_of(lax.rem(q, subs) * SUB, SUB), SUB)


class Block:
    def __init__(self, hbm, buf, sem, incoming):
        self.hbm, self.buf, self.sem, self.incoming = hbm, buf, sem, incoming

    def run(self, mat, rng, slot, act):
        hbm, buf, sem = self.hbm(mat, rng), self.buf.at[slot], self.sem.at[slot]
        pair = (hbm, buf) if self.incoming else (buf, hbm)
        act(pltpu.make_async_copy(*pair, sem))


class SplitBlock:
    def __init__(self, w_in, w_out, buf, buf_t, sem, incoming):
        self.w_in, self.w_out, self.buf, self.buf_t, self.sem, self.incoming = w_in, w_out, buf, buf_t, sem, incoming

    def run(self, mat, rng, slot, act):
        layer, odd = lax.div(mat, 2), lax.rem(mat, 2)

        def go(hbm, buf):
            pair = (hbm, buf) if self.incoming else (buf, hbm)
            act(pltpu.make_async_copy(*pair, self.sem.at[slot]))

        @pl.when(odd == 0)
        def _():
            go(self.w_in.at[layer, rng], self.buf.at[slot])

        @pl.when(odd == 1)
        def _():
            go(self.w_out.at[layer, :, rng], self.buf_t.at[slot])

    def take(self, mat, slot):
        @pl.when(lax.rem(mat, 2) == 1)
        def _():
            self.buf[slot] = self.buf_t[slot].T

    def give(self, mat, slot, value):
        @pl.when(lax.rem(mat, 2) == 0)
        def _():
            self.buf[slot] = value

        @pl.when(lax.rem(mat, 2) == 1)
        def _():
            self.buf_t[slot] = value.T


def stream(mats, subs, ins, outs, body, before=None):
    chunks = mats * subs

    def get(q):
        if before is not None:
            @pl.when(lax.rem(q, subs) == 0)
            def _():
                before(lax.div(q, subs))
        mat, rng = where(q, subs)
        for b in ins:
            b.run(mat, rng, lax.rem(q, DEPTH), lambda c: c.start())

    def put(q, act):
        mat, rng = where(q, subs)
        for b in outs:
            b.run(mat, rng, lax.rem(q, DEPTH), act)

    def early(q, carry):
        get(q)
        return carry
    lax.fori_loop(0, DEPTH - 1, early, 0)

    def one(q, carry):
        mat, rng = where(q, subs)
        slot = lax.rem(q, DEPTH)

        @pl.when(q + DEPTH - 1 < chunks)
        def _():
            get(q + DEPTH - 1)
        for b in ins:
            b.run(mat, rng, slot, lambda c: c.wait())

        @pl.when(q >= DEPTH)
        def _():
            put(q - DEPTH, lambda c: c.wait())
        body(mat, rng, slot)
        put(q, lambda c: c.start())
        return carry
    lax.fori_loop(0, chunks, one, 0)

    def late(q, carry):
        put(q, lambda c: c.wait())
        return carry
    lax.fori_loop(chunks - DEPTH, chunks, late, 0)


def neighbour_order():
    xpar, ypar = lax.rem(lax.axis_index('tx'), 2), lax.rem(lax.axis_index('ty'), 2)
    return 1 - xpar, xpar, 3 - ypar, 2 + ypar


def mix(v, bn, slot):
    for k in range(4):
        v = v + bn[k, slot].astype(f32)
    return v / 5.0


def rows_of(ref):
    return lambda mat, rng: ref.at[mat, rng]


def step_kernel(step, steps, names, *refs):
    r = dict(zip(names, refs))
    first, last, before_last = step == 0, step == steps, step == steps - 1
    x_ref, t_ref, nb, w, dw = r['x'], r['t'], r['nb'], r['w'], r['dw']
    mats, d, ff = w.shape
    rows = x_ref.shape[1]
    tiles = rows // TILE
    subs = d // SUB
    part_rows = d // PARTS
    per_set = mats * PARTS
    sems = r['copy_sem']
    send_sem, recv_sem = r['send_sem'], r['recv_sem']
    sets = nb.shape[0]
    slots = sets * per_set
    p_set = None if last else sets - 1
    y_set = None if first else 0
    order = neighbour_order()
    run = functools.partial(stream, mats, subs)
    block = (DEPTH, SUB, ff)

    tx, ty = lax.axis_index('tx'), lax.axis_index('ty')
    peers = (
        {'tx': tx + 1 - 2 * lax.rem(tx, 2)},
        {'tx': 3 - tx},
        {'ty': ty + 1 - 2 * lax.rem(ty, 2)},
        {'ty': lax.rem(ty + 2, 4)},
    )

    def remote(source, group, direction, mat, part):
        rng = pl.ds(pl.multiple_of(part * part_rows, part_rows), part_rows)
        slot = group * per_set + mat * PARTS + part
        src = nb.at[group, YDIR, mat, rng] if source is None else source.at[mat, rng]
        return pltpu.make_async_remote_copy(
            src_ref=src, dst_ref=nb.at[group, direction, mat, rng],
            send_sem=send_sem.at[direction, slot], recv_sem=recv_sem.at[direction, slot],
            device_id=peers[direction], device_id_type=pl.DeviceIdType.MESH)

    def send(source, group, mat):
        for part in range(PARTS):
            for direction in (YDIR, XDIR, CORE):
                remote(source, group, direction, mat, part).start()

    def arrived(group, mat, directions=(CORE, XDIR, ZDIR)):
        for part in range(PARTS):
            for direction in directions:
                remote(None, group, direction, mat, part).wait_recv()

    def forward(slot):
        group, rest = lax.div(slot, per_set), lax.rem(slot, per_set)
        mat, part = lax.div(rest, PARTS), lax.rem(rest, PARTS)
        remote(None, group, YDIR, mat, part).wait_recv()
        remote(None, group, ZDIR, mat, part).start()

    def loop(lo, hi, fn):
        def one(k, carry):
            fn(k)
            return carry
        lax.fori_loop(lo, hi, one, 0)

    def nb_blocks(source, group, buf):
        return [Block(lambda mat, rng, k=k: source.at[group, order[k], mat, rng], buf.at[k], sems.at[k], True)
                for k in range(4)]

    if not first:
        loop(0, mats, lambda mat: send(r['y_send'], y_set, mat))

    def late_send(mat, rng):
        if p_set is not None:
            @pl.when(jnp.logical_and(rng.start == 0, mat > 0))
            def _():
                send(w, p_set, mat - 1)

    if last:
        for mat in range(mats):
            pltpu.make_async_copy(r['pb'].at[mat], w.at[mat], sems.at[mat, 0]).start()
    elif first:
        def load_weights(bp, bt):
            src = SplitBlock(r['w_in'], r['w_out'], bp, bt, sems.at[4], True)

            def body(mat, rng, slot):
                src.take(mat, slot)
                w[mat, rng, :] = bp[slot].astype(bf16)
                late_send(mat, rng)
            run([src], [], body)
        pl.run_scoped(load_weights, pltpu.VMEM(block, f32), pltpu.VMEM((DEPTH, ff, SUB), f32))
    else:
        split = 'w_in' in r

        def new_weights(bp, bn, by, bo, bt=None):
            if split:
                src = SplitBlock(r['w_in'], r['w_out'], bp, bt, sems.at[4], True)
            else:
                src = Block(rows_of(r['p']), bp, sems.at[4], True)

            def body(mat, rng, slot):
                if split:
                    src.take(mat, slot)
                pn = mix(bp[slot], bn, slot) - LEARN_RATE * by[slot].astype(f32)
                bo[slot] = pn
                w[mat, rng, :] = pn.astype(bf16)
                late_send(mat, rng)
            ins = [src] + nb_blocks(r['p_nb'], r['p_nb'].shape[0] - 1, bn)
            ins += [Block(rows_of(r['y']), by, sems.at[5], True)]
            run(ins, [Block(rows_of(r['p_out']), bo, sems.at[6], False)], body)
        bufs = [pltpu.VMEM(block, f32), pltpu.VMEM((4,) + block, bf16), pltpu.VMEM(block, r['y'].dtype), pltpu.VMEM(block, f32)]
        if split:
            bufs.append(pltpu.VMEM((DEPTH, ff, SUB), f32))
        pl.run_scoped(new_weights, *bufs)

    def zero(k):
        mat, rng = where(k, subs)
        dw[mat, rng, :] = jnp.zeros((SUB, ff), f32)
    loop(0, mats * subs, zero)
    if p_set is not None:
        send(w, p_set, mats - 1)
    if last:
        for mat in range(mats):
            pltpu.make_async_copy(r['pb'].at[mat], w.at[mat], sems.at[mat, 0]).wait()

    layers = mats // 2
    inv_count = 1.0 / (rows * d)
    behind = 1 if first or last else 0

    def gradient(xb, tb, h_s, a_s, gp_s, dh_s):
        def fetch(i, slot):
            rng = pl.ds(pl.multiple_of(i * TILE, TILE), TILE)
            return (pltpu.make_async_copy(x_ref.at[step, rng], xb.at[slot], r['tile_sem'].at[0, slot]),
                    pltpu.make_async_copy(t_ref.at[step, rng], tb.at[slot], r['tile_sem'].at[1, slot]))
        for c in fetch(0, 0):
            c.start()

        def tile(i):
            slot = lax.rem(i, 2)
            if behind:
                @pl.when(i > 0)
                def _():
                    forward(PARTS * i - 1)
            else:
                forward(PARTS * i)
            for c in fetch(i, slot):
                c.wait()

            @pl.when(i + 1 < tiles)
            def _():
                for c in fetch(i + 1, 1 - slot):
                    c.start()
            h_s[0] = xb[slot]

            def fwd(l):
                h = h_s[l].astype(f32)
                inv = lax.rsqrt(jnp.mean(h * h, axis=-1, keepdims=True) + EPS)
                u = (h * inv).astype(bf16)
                acc = jnp.zeros((TILE, d), f32)
                for c in range(0, ff, COLS):
                    cs = slice(c, c + COLS)
                    z = dot_nn(u, w[2 * l, :, cs])
                    z2 = z * z
                    th = jnp.tanh(z * (GELU_A + GELU_B * z2))
                    s = 0.5 + 0.5 * th
                    a = (z * s).astype(bf16)
                    a_s[l, :, cs] = a
                    gp_s[l, :, cs] = s + (z * (0.5 * GELU_A + 1.5 * GELU_B * z2)) * (1.0 - th * th)
                    acc = acc + dot_nt(a, w[2 * l + 1, :, cs])
                h_s[l + 1] = (h + acc).astype(bf16)
            loop(0, layers, fwd)

            forward(PARTS * i + 1 - behind)
            err = h_s[layers].astype(f32) - tb[slot].astype(f32)
            dh_s[...] = ((err * inv_count) * 2.0).astype(bf16)

            def bwd(l, bottom):
                g = dh_s[...]
                g_t = g.T
                h = h_s[l].astype(f32)
                inv = lax.rsqrt(jnp.mean(h * h, axis=-1, keepdims=True) + EPS)
                u_t = (h * inv).astype(bf16).T
                du = jnp.zeros((TILE, d), f32)
                for c in range(0, ff, COLS):
                    cs = slice(c, c + COLS)
                    da = dot_nn(g, w[2 * l + 1, :, cs]).astype(bf16).astype(f32)
                    dz = (da * gp_s[l, :, cs]).astype(bf16)
                    dw[2 * l, :, cs] += dot_nn(u_t, dz)
                    dw[2 * l + 1, :, cs] += dot_nn(g_t, a_s[l, :, cs])
                    if not bottom:
                        du = du + dot_nt(dz, w[2 * l, :, cs])
                if not bottom:
                    du = du.astype(bf16).astype(f32)
                    dinv = jnp.sum(du * h, axis=-1, keepdims=True)
                    k = dinv * (inv * inv * inv) * (-1.0 / d)
                    dh_s[...] = (g.astype(f32) + du * inv + h * k).astype(bf16)

            loop(0, layers - 1, lambda q: bwd(layers - 1 - q, False))
            bwd(0, True)

        loop(0, tiles, tile)

    pl.run_scoped(gradient, pltpu.VMEM((2, TILE, d), bf16), pltpu.VMEM((2, TILE, d), bf16),
                  pltpu.VMEM((layers + 1, TILE, d), bf16), pltpu.VMEM((layers, TILE, ff), bf16),
                  pltpu.VMEM((layers, TILE, ff), f32), pltpu.VMEM((TILE, d), bf16))
    sent = tiles * PARTS - behind

    if first or last:
        forward(sent)
        sent += 1

        def keep_gradient(og):
            def body(mat, rng, slot):
                og[slot] = dw[mat, rng, :].astype(bf16)
            run([], [Block(rows_of(r['g_out']), og, sems.at[6], False)], body)
        pl.run_scoped(keep_gradient, pltpu.VMEM(block, bf16))
    else:
        forward(sent)
        forward(sent + 1)
        same = 'g' not in r

        def new_tracker(bn, by, bo, ob, og, bg=None):
            def before(mat):
                arrived(y_set, mat)
                for at, slot in ((3, sent + 2), (6, sent + 3)):
                    @pl.when(mat == at)
                    def _():
                        forward(slot)

            def body(mat, rng, slot):
                g = dw[mat, rng, :].astype(bf16)
                old = (by if same else bg)[slot].astype(f32)
                y = (mix(by[slot].astype(f32), bn, slot) + g.astype(f32)) - old
                bo[slot] = y
                ob[slot] = y.astype(bf16)
                og[slot] = g
            ins = [Block(rows_of(r['y']), by, sems.at[4], True)] + nb_blocks(nb, y_set, bn)
            if not same:
                ins += [Block(rows_of(r['g']), bg, sems.at[5], True)]
            outs = [Block(rows_of(r['y_out']), bo, sems.at[6], False),
                    Block(rows_of(r['yb_out']), ob, sems.at[7], False),
                    Block(rows_of(r['g_out']), og, sems.at[8], False)]
            run(ins, outs, body, before)
        bufs = [pltpu.VMEM((4,) + block, bf16), pltpu.VMEM(block, r['y'].dtype), pltpu.VMEM(block, f32),
                pltpu.VMEM(block, bf16), pltpu.VMEM(block, bf16)]
        if not same:
            bufs.append(pltpu.VMEM(block, bf16))
        pl.run_scoped(new_tracker, *bufs)
        sent += 4

    if before_last:
        def next_weights(bp, bn, by, bo, ob):
            def before(mat):
                for slot in range(PARTS):
                    nxt = p_set * per_set + (mat + 1) * PARTS + slot

                    @pl.when(jnp.logical_and(nxt >= sent, nxt < slots))
                    def _():
                        forward(nxt)
                arrived(p_set, mat)

            def body(mat, rng, slot):
                pn = mix(bp[slot], bn, slot) - LEARN_RATE * by[slot]
                bo[slot] = pn
                ob[slot] = pn.astype(bf16)
            ins = [Block(rows_of(r['p_out']), bp, sems.at[4], True)] + nb_blocks(nb, p_set, bn)
            ins += [Block(rows_of(r['y_out']), by, sems.at[5], True)]
            outs = [Block(rows_of(r['p_next']), bo, sems.at[6], False),
                    Block(rows_of(r['pb_next']), ob, sems.at[7], False)]
            run(ins, outs, body, before)
        pl.run_scoped(next_weights, pltpu.VMEM(block, f32), pltpu.VMEM((4,) + block, bf16), pltpu.VMEM(block, f32),
                      pltpu.VMEM(block, f32), pltpu.VMEM(block, bf16))
    else:
        loop(sent, slots, forward)
        loop(0, mats, lambda mat: arrived(y_set if last else p_set, mat))

    def drain(slot):
        group, rest = lax.div(slot, per_set), lax.rem(slot, per_set)
        for direction in range(4):
            remote(None, group, direction, lax.div(rest, PARTS), lax.rem(rest, PARTS)).wait_send()
    loop(0, slots, drain)


def final_kernel(p, y, nb, g_old, g, pi_out, po_out, yi_out, yo_out, bp, bn, by, bg, bh, bpo, bpt, byo, byt, sems):
    mats, d, _ = p.shape
    order = neighbour_order()
    p_dst = SplitBlock(pi_out, po_out, bpo, bpt, sems.at[8], False)
    y_dst = SplitBlock(yi_out, yo_out, byo, byt, sems.at[9], False)

    def body(mat, rng, slot):
        p_dst.give(mat, slot, bp[slot])
        new = (mix(by[slot], bn, slot) + bh[slot].astype(f32)) - bg[slot].astype(f32)
        y_dst.give(mat, slot, new)
    ins = [Block(rows_of(p), bp, sems.at[4], True), Block(rows_of(y), by, sems.at[5], True),
           Block(rows_of(g_old), bg, sems.at[6], True), Block(rows_of(g), bh, sems.at[7], True)]
    ins += [Block(lambda mat, rng, k=k: nb.at[0, order[k], mat, rng], bn.at[k], sems.at[k], True) for k in range(4)]
    stream(mats, d // SUB, ins, [p_dst, y_dst], body)


ANY = pl.BlockSpec(memory_space=pl.ANY)
VMEM_LIMIT = 67043328


def run_step(step, steps, dims, ins):
    mats, d, ff = dims
    first, last = step == 0, step == steps
    sets = 1 if first or last else 2
    big = lambda dtype: jax.ShapeDtypeStruct(dims, dtype)
    outs = {'nb': jax.ShapeDtypeStruct((sets, 4, mats, d, ff), bf16), 'g_out': big(bf16)}
    if not first and not last:
        outs.update(p_out=big(f32), y_out=big(f32), yb_out=big(bf16))
    if step == steps - 1:
        outs.update(p_next=big(f32), pb_next=big(bf16))
    scratch = {
        'w': pltpu.VMEM(dims, bf16),
        'dw': pltpu.VMEM(dims, f32),
        'send_sem': pltpu.SemaphoreType.DMA((4, sets * mats * PARTS)),
        'recv_sem': pltpu.SemaphoreType.DMA((4, sets * mats * PARTS)),
        'copy_sem': pltpu.SemaphoreType.DMA((9, DEPTH)),
        'tile_sem': pltpu.SemaphoreType.DMA((2, 2)),
    }
    names = tuple(ins) + tuple(outs) + tuple(scratch)
    res = pl.pallas_call(
        functools.partial(step_kernel, step, steps, names),
        out_shape=tuple(outs.values()),
        in_specs=[ANY] * len(ins),
        out_specs=tuple(ANY for _ in outs),
        scratch_shapes=list(scratch.values()),
        compiler_params=pltpu.CompilerParams(vmem_limit_bytes=VMEM_LIMIT, has_side_effects=True),
        name='step%d' % step,
    )(*ins.values())
    return dict(zip(outs, res))


def finish(layers, p, y, nb, g_old, g):
    mats, d, ff = p.shape
    block = (DEPTH, SUB, ff)
    block_t = (DEPTH, ff, SUB)
    w_in, w_out = jax.ShapeDtypeStruct((layers, d, ff), f32), jax.ShapeDtypeStruct((layers, ff, d), f32)
    return pl.pallas_call(
        final_kernel,
        out_shape=(w_in, w_out, w_in, w_out),
        in_specs=[ANY] * 5,
        out_specs=(ANY,) * 4,
        scratch_shapes=[pltpu.VMEM(block, f32), pltpu.VMEM((4,) + block, bf16), pltpu.VMEM(block, f32),
                        pltpu.VMEM(block, bf16), pltpu.VMEM(block, bf16),
                        pltpu.VMEM(block, f32), pltpu.VMEM(block_t, f32), pltpu.VMEM(block, f32), pltpu.VMEM(block_t, f32),
                        pltpu.SemaphoreType.DMA((10, DEPTH))],
        compiler_params=pltpu.CompilerParams(vmem_limit_bytes=VMEM_LIMIT),
        name='finish',
    )(p, y, nb, g_old, g)


def solution(mesh):
    def device_fn(w_in, w_out, inputs, targets):
        w_in, w_out = w_in[0, 0], w_out[0, 0]
        layers, d, ff = w_in.shape
        dims = (2 * layers, d, ff)
        data = {'x': inputs[0, 0], 't': targets[0, 0]}
        steps = data['x'].shape[0] - 1
        out = run_step(0, steps, dims, {**data, 'w_in': w_in, 'w_out': w_out})
        g0 = out['g_out']
        out = run_step(1, steps, dims, {**data, 'w_in': w_in, 'w_out': w_out, 'p_nb': out['nb'], 'y': g0, 'y_send': g0})
        for step in range(2, steps):
            out = run_step(step, steps, dims, {**data, 'p': out['p_out'], 'p_nb': out['nb'], 'y': out['y_out'],
                                               'y_send': out['yb_out'], 'g': out['g_out']})
        end = run_step(steps, steps, dims, {**data, 'pb': out['pb_next'], 'y_send': out['yb_out']})
        res = finish(layers, out['p_next'], out['y_out'], end['nb'], out['g_out'], end['g_out'])
        return tuple(v[None, None] for v in res)

    spec = P('tx', 'ty')
    return jax.shard_map(device_fn, mesh=mesh, in_specs=(spec,) * 4, out_specs=(spec,) * 4, check_vma=False)
```

```python
import functools

import jax
import jax.numpy as jnp
import numpy as np
from jax import lax
from jax.experimental import pallas as pl
from jax.experimental.pallas import tpu as pltpu
from jax.sharding import PartitionSpec as P

bf16, f32 = jnp.bfloat16, jnp.float32
EPS = 1e-6
LEARN_RATE = 0.125
GELU_A = float(np.sqrt(2 / np.pi))
GELU_B = GELU_A * 0.044715
TILE = 512
COLS = 768
SUB = 128
DEPTH = 4
PARTS = 2
CORE, XDIR, YDIR, ZDIR = range(4)


def dot_nt(a, b):
    return lax.dot_general(a, b, (((1,), (1,)), ((), ())), preferred_element_type=f32)


def dot_nn(a, b):
    return jnp.dot(a, b, preferred_element_type=f32)


def where(q, subs):
    return lax.div(q, subs), pl.ds(pl.multiple_of(lax.rem(q, subs) * SUB, SUB), SUB)


class Block:
    def __init__(self, hbm, buf, sem, incoming):
        self.hbm, self.buf, self.sem, self.incoming = hbm, buf, sem, incoming

    def run(self, mat, rng, slot, act):
        hbm, buf, sem = self.hbm(mat, rng), self.buf.at[slot], self.sem.at[slot]
        pair = (hbm, buf) if self.incoming else (buf, hbm)
        act(pltpu.make_async_copy(*pair, sem))


class SplitBlock:
    def __init__(self, w_in, w_out, buf, buf_t, sem, incoming):
        self.w_in, self.w_out, self.buf, self.buf_t, self.sem, self.incoming = w_in, w_out, buf, buf_t, sem, incoming

    def run(self, mat, rng, slot, act):
        layer, odd = lax.div(mat, 2), lax.rem(mat, 2)

        def go(hbm, buf):
            pair = (hbm, buf) if self.incoming else (buf, hbm)
            act(pltpu.make_async_copy(*pair, self.sem.at[slot]))

        @pl.when(odd == 0)
        def _():
            go(self.w_in.at[layer, rng], self.buf.at[slot])

        @pl.when(odd == 1)
        def _():
            go(self.w_out.at[layer, :, rng], self.buf_t.at[slot])

    def take(self, mat, slot):
        @pl.when(lax.rem(mat, 2) == 1)
        def _():
            self.buf[slot] = self.buf_t[slot].T

    def give(self, mat, slot, value):
        @pl.when(lax.rem(mat, 2) == 0)
        def _():
            self.buf[slot] = value

        @pl.when(lax.rem(mat, 2) == 1)
        def _():
            self.buf_t[slot] = value.T


def stream(mats, subs, ins, outs, body, before=None):
    chunks = mats * subs

    def get(q):
        if before is not None:
            @pl.when(lax.rem(q, subs) == 0)
            def _():
                before(lax.div(q, subs))
        mat, rng = where(q, subs)
        for b in ins:
            b.run(mat, rng, lax.rem(q, DEPTH), lambda c: c.start())

    def put(q, act):
        mat, rng = where(q, subs)
        for b in outs:
            b.run(mat, rng, lax.rem(q, DEPTH), act)

    def early(q, carry):
        get(q)
        return carry
    lax.fori_loop(0, DEPTH - 1, early, 0)

    def one(q, carry):
        mat, rng = where(q, subs)
        slot = lax.rem(q, DEPTH)

        @pl.when(q + DEPTH - 1 < chunks)
        def _():
            get(q + DEPTH - 1)
        for b in ins:
            b.run(mat, rng, slot, lambda c: c.wait())

        @pl.when(q >= DEPTH)
        def _():
            put(q - DEPTH, lambda c: c.wait())
        body(mat, rng, slot)
        put(q, lambda c: c.start())
        return carry
    lax.fori_loop(0, chunks, one, 0)

    def late(q, carry):
        put(q, lambda c: c.wait())
        return carry
    lax.fori_loop(chunks - DEPTH, chunks, late, 0)


def neighbour_order():
    xpar, ypar = lax.rem(lax.axis_index('tx'), 2), lax.rem(lax.axis_index('ty'), 2)
    return 1 - xpar, xpar, 3 - ypar, 2 + ypar


def mix(v, bn, slot):
    for k in range(4):
        v = v + bn[k, slot].astype(f32)
    return v / 5.0


def rows_of(ref):
    return lambda mat, rng: ref.at[mat, rng]


def step_kernel(step, steps, names, *refs):
    r = dict(zip(names, refs))
    first, last, before_last = step == 0, step == steps, step == steps - 1
    x_ref, t_ref, nb, w, dw = r['x'], r['t'], r['nb'], r['w'], r['dw']
    mats, d, ff = w.shape
    rows = x_ref.shape[1]
    tiles = rows // TILE
    subs = d // SUB
    part_rows = d // PARTS
    per_set = mats * PARTS
    sems = r['copy_sem']
    send_sem, recv_sem = r['send_sem'], r['recv_sem']
    sets = nb.shape[0]
    slots = sets * per_set
    p_set = None if last else sets - 1
    y_set = None if first else 0
    order = neighbour_order()
    run = functools.partial(stream, mats, subs)
    block = (DEPTH, SUB, ff)

    tx, ty = lax.axis_index('tx'), lax.axis_index('ty')
    peers = (
        {'tx': tx + 1 - 2 * lax.rem(tx, 2)},
        {'tx': 3 - tx},
        {'ty': ty + 1 - 2 * lax.rem(ty, 2)},
        {'ty': lax.rem(ty + 2, 4)},
    )

    def remote(source, group, direction, mat, part):
        rng = pl.ds(pl.multiple_of(part * part_rows, part_rows), part_rows)
        slot = group * per_set + mat * PARTS + part
        src = nb.at[group, YDIR, mat, rng] if source is None else source.at[mat, rng]
        return pltpu.make_async_remote_copy(
            src_ref=src, dst_ref=nb.at[group, direction, mat, rng],
            send_sem=send_sem.at[direction, slot], recv_sem=recv_sem.at[direction, slot],
            device_id=peers[direction], device_id_type=pl.DeviceIdType.MESH)

    def send(source, group, mat):
        for part in range(PARTS):
            for direction in (YDIR, XDIR, CORE):
                remote(source, group, direction, mat, part).start()

    def arrived(group, mat, directions=(CORE, XDIR, ZDIR)):
        for part in range(PARTS):
            for direction in directions:
                remote(None, group, direction, mat, part).wait_recv()

    def forward(slot):
        group, rest = lax.div(slot, per_set), lax.rem(slot, per_set)
        mat, part = lax.div(rest, PARTS), lax.rem(rest, PARTS)
        remote(None, group, YDIR, mat, part).wait_recv()
        remote(None, group, ZDIR, mat, part).start()

    def loop(lo, hi, fn):
        def one(k, carry):
            fn(k)
            return carry
        lax.fori_loop(lo, hi, one, 0)

    def nb_blocks(source, group, buf):
        return [Block(lambda mat, rng, k=k: source.at[group, order[k], mat, rng], buf.at[k], sems.at[k], True)
                for k in range(4)]

    if not first:
        loop(0, mats, lambda mat: send(r['y_send'], y_set, mat))

    def late_send(mat, rng):
        if p_set is not None:
            @pl.when(jnp.logical_and(rng.start == 0, mat > 0))
            def _():
                send(w, p_set, mat - 1)

    if last:
        for mat in range(mats):
            pltpu.make_async_copy(r['pb'].at[mat], w.at[mat], sems.at[mat, 0]).start()
    elif first:
        def load_weights(bp, bt):
            src = SplitBlock(r['w_in'], r['w_out'], bp, bt, sems.at[4], True)

            def body(mat, rng, slot):
                src.take(mat, slot)
                w[mat, rng, :] = bp[slot].astype(bf16)
                late_send(mat, rng)
            run([src], [], body)
        pl.run_scoped(load_weights, pltpu.VMEM(block, f32), pltpu.VMEM((DEPTH, ff, SUB), f32))
    else:
        split = 'w_in' in r

        def first_forward(mat):
            @pl.when(mat == 5)
            def _():
                forward(0)

        def new_weights(bp, bn, by, bo, bt=None):
            if split:
                src = SplitBlock(r['w_in'], r['w_out'], bp, bt, sems.at[4], True)
            else:
                src = Block(rows_of(r['p']), bp, sems.at[4], True)

            def body(mat, rng, slot):
                if split:
                    src.take(mat, slot)
                pn = mix(bp[slot], bn, slot) - LEARN_RATE * by[slot].astype(f32)
                bo[slot] = pn
                w[mat, rng, :] = pn.astype(bf16)
                late_send(mat, rng)
            ins = [src] + nb_blocks(r['p_nb'], r['p_nb'].shape[0] - 1, bn)
            ins += [Block(rows_of(r['y']), by, sems.at[5], True)]
            run(ins, [Block(rows_of(r['p_out']), bo, sems.at[6], False)], body, first_forward)
        bufs = [pltpu.VMEM(block, f32), pltpu.VMEM((4,) + block, bf16), pltpu.VMEM(block, r['y'].dtype), pltpu.VMEM(block, f32)]
        if split:
            bufs.append(pltpu.VMEM((DEPTH, ff, SUB), f32))
        pl.run_scoped(new_weights, *bufs)

    def zero(k):
        mat, rng = where(k, subs)
        dw[mat, rng, :] = jnp.zeros((SUB, ff), f32)
    loop(0, mats * subs, zero)
    if p_set is not None:
        send(w, p_set, mats - 1)
    if last:
        for mat in range(mats):
            pltpu.make_async_copy(r['pb'].at[mat], w.at[mat], sems.at[mat, 0]).wait()

    layers = mats // 2
    inv_count = 1.0 / (rows * d)
    behind = 1 if first or last else -1

    def gradient(xb, tb, h_s, a_s, gp_s, dh_s):
        def fetch(i, slot):
            rng = pl.ds(pl.multiple_of(i * TILE, TILE), TILE)
            return (pltpu.make_async_copy(x_ref.at[step, rng], xb.at[slot], r['tile_sem'].at[0, slot]),
                    pltpu.make_async_copy(t_ref.at[step, rng], tb.at[slot], r['tile_sem'].at[1, slot]))
        for c in fetch(0, 0):
            c.start()

        def tile(i):
            slot = lax.rem(i, 2)
            if behind > 0:
                @pl.when(i > 0)
                def _():
                    forward(PARTS * i - 1)
            else:
                forward(PARTS * i + 1)
            for c in fetch(i, slot):
                c.wait()

            @pl.when(i + 1 < tiles)
            def _():
                for c in fetch(i + 1, 1 - slot):
                    c.start()
            h_s[0] = xb[slot]

            def fwd(l):
                h = h_s[l].astype(f32)
                inv = lax.rsqrt(jnp.mean(h * h, axis=-1, keepdims=True) + EPS)
                u = (h * inv).astype(bf16)
                acc = jnp.zeros((TILE, d), f32)
                for c in range(0, ff, COLS):
                    cs = slice(c, c + COLS)
                    z = dot_nn(u, w[2 * l, :, cs])
                    z2 = z * z
                    th = jnp.tanh(z * (GELU_A + GELU_B * z2))
                    s = 0.5 + 0.5 * th
                    a = (z * s).astype(bf16)
                    a_s[l, :, cs] = a
                    gp_s[l, :, cs] = s + (z * (0.5 * GELU_A + 1.5 * GELU_B * z2)) * (1.0 - th * th)
                    acc = acc + dot_nt(a, w[2 * l + 1, :, cs])
                h_s[l + 1] = (h + acc).astype(bf16)
            loop(0, layers, fwd)

            forward(PARTS * i + 1 - behind)
            err = h_s[layers].astype(f32) - tb[slot].astype(f32)
            dh_s[...] = ((err * inv_count) * 2.0).astype(bf16)

            def bwd(l, bottom):
                g = dh_s[...]
                g_t = g.T
                h = h_s[l].astype(f32)
                inv = lax.rsqrt(jnp.mean(h * h, axis=-1, keepdims=True) + EPS)
                u_t = (h * inv).astype(bf16).T
                du = jnp.zeros((TILE, d), f32)
                for c in range(0, ff, COLS):
                    cs = slice(c, c + COLS)
                    da = dot_nn(g, w[2 * l + 1, :, cs]).astype(bf16).astype(f32)
                    dz = (da * gp_s[l, :, cs]).astype(bf16)
                    dw[2 * l, :, cs] += dot_nn(u_t, dz)
                    dw[2 * l + 1, :, cs] += dot_nn(g_t, a_s[l, :, cs])
                    if not bottom:
                        du = du + dot_nt(dz, w[2 * l, :, cs])
                if not bottom:
                    du = du.astype(bf16).astype(f32)
                    dinv = jnp.sum(du * h, axis=-1, keepdims=True)
                    k = dinv * (inv * inv * inv) * (-1.0 / d)
                    dh_s[...] = (g.astype(f32) + du * inv + h * k).astype(bf16)

            shared = 0 if first or last else 1
            loop(0, layers - 1 + shared, lambda q: bwd(layers - 1 - q, False))
            if not shared:
                @pl.when(i == tiles - 1)
                def _():
                    forward(PARTS * tiles - 1)
                bwd(0, True)

        loop(0, tiles, tile)

    pl.run_scoped(gradient, pltpu.VMEM((2, TILE, d), bf16), pltpu.VMEM((2, TILE, d), bf16),
                  pltpu.VMEM((layers + 1, TILE, d), bf16), pltpu.VMEM((layers, TILE, ff), bf16),
                  pltpu.VMEM((layers, TILE, ff), f32), pltpu.VMEM((TILE, d), bf16))
    sent = tiles * PARTS - behind

    if first or last:
        sent += 1

        def keep_gradient(og):
            def body(mat, rng, slot):
                og[slot] = dw[mat, rng, :].astype(bf16)
            run([], [Block(rows_of(r['g_out']), og, sems.at[6], False)], body)
        pl.run_scoped(keep_gradient, pltpu.VMEM(block, bf16))
    else:
        forward(sent)
        forward(sent + 1)
        same = 'g' not in r

        def new_tracker(bn, by, bo, ob, og, bg=None):
            def before(mat):
                arrived(y_set, mat)
                for at, slot in ((3, sent + 2), (6, sent + 3)):
                    @pl.when(mat == at)
                    def _():
                        forward(slot)

            def body(mat, rng, slot):
                g = dw[mat, rng, :].astype(bf16)
                old = (by if same else bg)[slot].astype(f32)
                y = (mix(by[slot].astype(f32), bn, slot) + g.astype(f32)) - old
                bo[slot] = y
                ob[slot] = y.astype(bf16)
                og[slot] = g
            ins = [Block(rows_of(r['y']), by, sems.at[4], True)] + nb_blocks(nb, y_set, bn)
            if not same:
                ins += [Block(rows_of(r['g']), bg, sems.at[5], True)]
            outs = [Block(rows_of(r['y_out']), bo, sems.at[6], False),
                    Block(rows_of(r['yb_out']), ob, sems.at[7], False),
                    Block(rows_of(r['g_out']), og, sems.at[8], False)]
            run(ins, outs, body, before)
        bufs = [pltpu.VMEM((4,) + block, bf16), pltpu.VMEM(block, r['y'].dtype), pltpu.VMEM(block, f32),
                pltpu.VMEM(block, bf16), pltpu.VMEM(block, bf16)]
        if not same:
            bufs.append(pltpu.VMEM(block, bf16))
        pl.run_scoped(new_tracker, *bufs)
        sent += 4

    if before_last:
        def next_weights(bp, bn, by, bo, ob):
            def before(mat):
                for slot in range(PARTS):
                    nxt = p_set * per_set + (mat + 1) * PARTS + slot

                    @pl.when(jnp.logical_and(nxt >= sent, nxt < slots))
                    def _():
                        forward(nxt)
                arrived(p_set, mat)

            def body(mat, rng, slot):
                pn = mix(bp[slot], bn, slot) - LEARN_RATE * by[slot]
                bo[slot] = pn
                ob[slot] = pn.astype(bf16)
            ins = [Block(rows_of(r['p_out']), bp, sems.at[4], True)] + nb_blocks(nb, p_set, bn)
            ins += [Block(rows_of(r['y_out']), by, sems.at[5], True)]
            outs = [Block(rows_of(r['p_next']), bo, sems.at[6], False),
                    Block(rows_of(r['pb_next']), ob, sems.at[7], False)]
            run(ins, outs, body, before)
        pl.run_scoped(next_weights, pltpu.VMEM(block, f32), pltpu.VMEM((4,) + block, bf16), pltpu.VMEM(block, f32),
                      pltpu.VMEM(block, f32), pltpu.VMEM(block, bf16))
    else:
        loop(sent, slots, forward)
        loop(0, mats, lambda mat: arrived(y_set if last else p_set, mat))

    def drain(slot):
        group, rest = lax.div(slot, per_set), lax.rem(slot, per_set)
        for direction in range(4):
            remote(None, group, direction, lax.div(rest, PARTS), lax.rem(rest, PARTS)).wait_send()
    loop(0, slots, drain)


def final_kernel(p, y, nb, g_old, g, pi_out, po_out, yi_out, yo_out, bp, bn, by, bg, bh, bpo, bpt, byo, byt, sems):
    mats, d, _ = p.shape
    order = neighbour_order()
    p_dst = SplitBlock(pi_out, po_out, bpo, bpt, sems.at[8], False)
    y_dst = SplitBlock(yi_out, yo_out, byo, byt, sems.at[9], False)

    def body(mat, rng, slot):
        p_dst.give(mat, slot, bp[slot])
        new = (mix(by[slot], bn, slot) + bh[slot].astype(f32)) - bg[slot].astype(f32)
        y_dst.give(mat, slot, new)
    ins = [Block(rows_of(p), bp, sems.at[4], True), Block(rows_of(y), by, sems.at[5], True),
           Block(rows_of(g_old), bg, sems.at[6], True), Block(rows_of(g), bh, sems.at[7], True)]
    ins += [Block(lambda mat, rng, k=k: nb.at[0, order[k], mat, rng], bn.at[k], sems.at[k], True) for k in range(4)]
    stream(mats, d // SUB, ins, [p_dst, y_dst], body)


ANY = pl.BlockSpec(memory_space=pl.ANY)
VMEM_LIMIT = 67043328


def run_step(step, steps, dims, ins):
    mats, d, ff = dims
    first, last = step == 0, step == steps
    sets = 1 if first or last else 2
    big = lambda dtype: jax.ShapeDtypeStruct(dims, dtype)
    outs = {'nb': jax.ShapeDtypeStruct((sets, 4, mats, d, ff), bf16), 'g_out': big(bf16)}
    if not first and not last:
        outs.update(p_out=big(f32), y_out=big(f32), yb_out=big(bf16))
    if step == steps - 1:
        outs.update(p_next=big(f32), pb_next=big(bf16))
    scratch = {
        'w': pltpu.VMEM(dims, bf16),
        'dw': pltpu.VMEM(dims, f32),
        'send_sem': pltpu.SemaphoreType.DMA((4, sets * mats * PARTS)),
        'recv_sem': pltpu.SemaphoreType.DMA((4, sets * mats * PARTS)),
        'copy_sem': pltpu.SemaphoreType.DMA((9, DEPTH)),
        'tile_sem': pltpu.SemaphoreType.DMA((2, 2)),
    }
    names = tuple(ins) + tuple(outs) + tuple(scratch)
    res = pl.pallas_call(
        functools.partial(step_kernel, step, steps, names),
        out_shape=tuple(outs.values()),
        in_specs=[ANY] * len(ins),
        out_specs=tuple(ANY for _ in outs),
        scratch_shapes=list(scratch.values()),
        compiler_params=pltpu.CompilerParams(vmem_limit_bytes=VMEM_LIMIT, has_side_effects=True),
        name='step%d' % step,
    )(*ins.values())
    return dict(zip(outs, res))


def finish(layers, p, y, nb, g_old, g):
    mats, d, ff = p.shape
    block = (DEPTH, SUB, ff)
    block_t = (DEPTH, ff, SUB)
    w_in, w_out = jax.ShapeDtypeStruct((layers, d, ff), f32), jax.ShapeDtypeStruct((layers, ff, d), f32)
    return pl.pallas_call(
        final_kernel,
        out_shape=(w_in, w_out, w_in, w_out),
        in_specs=[ANY] * 5,
        out_specs=(ANY,) * 4,
        scratch_shapes=[pltpu.VMEM(block, f32), pltpu.VMEM((4,) + block, bf16), pltpu.VMEM(block, f32),
                        pltpu.VMEM(block, bf16), pltpu.VMEM(block, bf16),
                        pltpu.VMEM(block, f32), pltpu.VMEM(block_t, f32), pltpu.VMEM(block, f32), pltpu.VMEM(block_t, f32),
                        pltpu.SemaphoreType.DMA((10, DEPTH))],
        compiler_params=pltpu.CompilerParams(vmem_limit_bytes=VMEM_LIMIT),
        name='finish',
    )(p, y, nb, g_old, g)


def solution(mesh):
    def device_fn(w_in, w_out, inputs, targets):
        w_in, w_out = w_in[0, 0], w_out[0, 0]
        layers, d, ff = w_in.shape
        dims = (2 * layers, d, ff)
        data = {'x': inputs[0, 0], 't': targets[0, 0]}
        steps = data['x'].shape[0] - 1
        out = run_step(0, steps, dims, {**data, 'w_in': w_in, 'w_out': w_out})
        g0 = out['g_out']
        out = run_step(1, steps, dims, {**data, 'w_in': w_in, 'w_out': w_out, 'p_nb': out['nb'], 'y': g0, 'y_send': g0})
        for step in range(2, steps):
            out = run_step(step, steps, dims, {**data, 'p': out['p_out'], 'p_nb': out['nb'], 'y': out['y_out'],
                                               'y_send': out['yb_out'], 'g': out['g_out']})
        end = run_step(steps, steps, dims, {**data, 'pb': out['pb_next'], 'y_send': out['yb_out']})
        res = finish(layers, out['p_next'], out['y_out'], end['nb'], out['g_out'], end['g_out'])
        return tuple(v[None, None] for v in res)

    spec = P('tx', 'ty')
    return jax.shard_map(device_fn, mesh=mesh, in_specs=(spec,) * 4, out_specs=(spec,) * 4, check_vma=False)
```
